8 devices in a mesh: rep: 2 (over z, y), vocab: 4 (over x, core).
Axes of the slice: x: 2, y: 2, z: 1, core: 2. Of those that a mesh axis runs over, the one named last changes fastest.
Arguments:
- hidden: bfloat16 [512, 5120], P(('rep', 'vocab')), parts along dimension 0
- w_head: bfloat16 [131072, 5120], P('vocab')
- allowed_ids: int32 [4096], P('rep'), parts along dimension 0
- allowed_valid: int32 [4096], P('rep'), parts along dimension 0
- target_pos: int32 [512], P(('rep', 'vocab')), parts along dimension 0
Outputs:
- output 1: float32 [512, 2048], P(('rep', 'vocab')), parts along dimension 0
- output 2: float32 [512], P(('rep', 'vocab')), parts along dimension 0
There are 2 independent parts. The reference program is written for one: setup_inputs(seed, part) draws one part's arguments, and reference() takes and returns one part's arrays. A program takes and returns all parts, laid end to end along the dimension named above; an argument that names none is the same for every part.
All inputs are finite; a program needn't handle non-finite values.
Results may differ from the reference program's by a relative error of at most 0.001.
Values are sent between devices in bfloat16 or wider.
A program may use at most 1.5 GiB of HBM per device.

```python
import jax
import jax.numpy as jnp
from jax import lax

VOCAB_SIZE = 131072
MODEL_DIM = 5120
LIST_LEN = 2048
BATCH_ROWS = 256
SHARDS = 4
HEAD_BLOCKS = 128
INV_TEMP = 1.25


def draw_head(key_head):
    block_keys = jax.random.split(key_head, HEAD_BLOCKS)
    row_scale = MODEL_DIM ** -0.5

    def one_block(block_key):
        block_vals = jax.random.normal(block_key, (VOCAB_SIZE // HEAD_BLOCKS, MODEL_DIM), jnp.float32)
        return (block_vals * row_scale).astype(jnp.bfloat16)

    return lax.map(one_block, block_keys).reshape(VOCAB_SIZE, MODEL_DIM)


def draw_list(key_list):
    key_pair, key_move, key_offset, key_order, key_count, key_valid, key_target = jax.random.split(key_list, 7)
    per_shard = LIST_LEN // SHARDS
    slot_cap = 2 * per_shard
    vocab_local = VOCAB_SIZE // SHARDS
    shard_order = jax.random.permutation(key_pair, SHARDS)
    move_sizes = jax.random.randint(key_move, (SHARDS // 2,), 0, per_shard + 1).at[0].set(per_shard)
    shard_gain = jnp.zeros((SHARDS,), jnp.int32).at[shard_order[0::2]].set(move_sizes).at[shard_order[1::2]].set(-move_sizes)
    counts = per_shard + shard_gain
    offset_keys = jax.random.split(key_offset, SHARDS)
    offsets = jax.vmap(lambda one_key: jax.random.permutation(one_key, vocab_local)[:slot_cap])(offset_keys)
    candidates = jnp.arange(SHARDS, dtype=jnp.int32)[:, None] * vocab_local + offsets
    keep_slot = jnp.arange(slot_cap)[None, :] < counts[:, None]
    sort_key = jnp.where(keep_slot, 0, 1) * (SHARDS * slot_cap) + jnp.arange(SHARDS * slot_cap).reshape(SHARDS, slot_cap)
    chosen = jnp.argsort(sort_key.reshape(-1))[:LIST_LEN]
    grouped = candidates.reshape(-1)[chosen]
    allowed_ids = grouped[jax.random.permutation(key_order, LIST_LEN)].astype(jnp.int32)
    valid_count = jax.random.randint(key_count, (), LIST_LEN // 2, LIST_LEN + 1)
    valid_perm = jax.random.permutation(key_valid, LIST_LEN)
    allowed_valid = (valid_perm < valid_count).astype(jnp.int32)
    inverse = jnp.argsort(valid_perm)
    pick_rank = jax.random.randint(key_target, (BATCH_ROWS,), 0, valid_count)
    target_pos = inverse[pick_rank].astype(jnp.int32)
    return allowed_ids, allowed_valid, target_pos


def setup_inputs(seed: int = 0, part: int = 0) -> dict:
    root_key = jax.random.key(seed)
    key_head, key_groups = jax.random.split(root_key)
    key_part = jax.random.fold_in(key_groups, part)
    key_hidden, key_list = jax.random.split(key_part)
    hidden = jax.random.normal(key_hidden, (BATCH_ROWS, MODEL_DIM), jnp.float32).astype(jnp.bfloat16)
    allowed_ids, allowed_valid, target_pos = draw_list(key_list)
    return dict(hidden=hidden, w_head=draw_head(key_head), allowed_ids=allowed_ids, allowed_valid=allowed_valid, target_pos=target_pos)


def reference(hidden, w_head, allowed_ids, allowed_valid, target_pos):
    head_rows = jnp.take(w_head, allowed_ids, axis=0)
    scores = jnp.dot(hidden, head_rows.T, preferred_element_type=jnp.float32) * INV_TEMP
    keep_mask = (allowed_valid > 0)[None, :]
    masked = jnp.where(keep_mask, scores, -jnp.inf)
    log_norm = jax.nn.logsumexp(masked, axis=1)
    token_probs = jnp.where(keep_mask, jnp.exp(masked - log_norm[:, None]), 0.0)
    picked = jnp.take_along_axis(scores, target_pos[:, None], axis=1)[:, 0]
    return token_probs, picked - log_norm
```

```python
import functools

import jax
import jax.numpy as jnp
from jax import lax
from jax.experimental import pallas as pl
from jax.experimental.pallas import tpu as pltpu
from jax.sharding import PartitionSpec as P

INV_TEMP = 1.25
MESH = pl.DeviceIdType.MESH
LANES = 128
TILE_ROWS = 8
CHUNK = 128
BUFS = 3
UNROLL = 8
PARTS = 4


def gather_dot_kernel(keys, count, w, h_own, h_pair, h_far, h_far_pair, s_out, pairs, hidden, res, h_sem, sem, *, row_bits, trash):
    core = lax.rem(lax.axis_index('vocab'), 2)
    rows_dev = h_own.shape[0]
    ktiles = w.shape[1]
    base_own = pl.multiple_of(core * rows_dev, rows_dev)
    base_pair = pl.multiple_of((1 - core) * rows_dev, rows_dev)
    copies = []
    for i, (src, base) in enumerate(((h_own, base_own), (h_pair, base_pair), (h_far, 2 * rows_dev + base_own), (h_far_pair, 2 * rows_dev + base_pair))):
        copies.append(pltpu.make_async_copy(src, hidden.at[pl.ds(pl.multiple_of(base, rows_dev), rows_dev)], h_sem.at[i]))
        copies[-1].start()
    n = count[0]
    n_chunks = lax.div(n + CHUNK - 1, CHUNK)

    def start(c):
        slot = lax.rem(c, BUFS)

        def issue(i, carry):
            for u in range(UNROLL):
                j = i * UNROLL + u
                row = lax.bitwise_and(keys[c * CHUNK + j], (1 << row_bits) - 1)
                src = w.at[lax.shift_right_logical(row, 3), :, lax.bitwise_and(lax.shift_right_logical(row, 1), 3)]
                pltpu.make_async_copy(src, pairs.at[slot, :, j], sem.at[slot]).start()
            return carry

        lax.fori_loop(0, CHUNK // UNROLL, issue, 0)

    for c in range(BUFS - 1):
        @pl.when(c < n_chunks)
        def _():
            start(c)

    def zero(i, carry):
        s_out[pl.ds(pl.multiple_of(i * 64, 64), 64), :] = jnp.zeros((64, s_out.shape[1]), jnp.float32)
        return carry

    lax.fori_loop(0, trash // 64, zero, 0)
    for copy in copies:
        copy.wait()

    def body(c, carry):
        slot = lax.rem(c, BUFS)

        @pl.when(c + BUFS - 1 < n_chunks)
        def _():
            start(c + BUFS - 1)

        pltpu.make_async_copy(pairs.at[slot], pairs.at[slot], sem.at[slot]).wait()
        acc = jnp.zeros((2 * CHUNK, hidden.shape[0]), jnp.float32)
        for k in range(ktiles // 2):
            lhs = jnp.concatenate([pairs[slot, 2 * k + d].reshape(2 * CHUNK, LANES) for d in range(2)], axis=1)
            acc += lax.dot_general(lhs, hidden[:, k * 2 * LANES:(k + 1) * 2 * LANES], (((1,), (1,)), ((), ())), preferred_element_type=jnp.float32)
        res[...] = acc

        def scatter(i, carry):
            for u in range(UNROLL):
                j = i * UNROLL + u
                key = keys[c * CHUNK + j]
                pos = jnp.minimum(lax.shift_right_logical(key, row_bits), trash)
                s_out[pl.ds(pos, 1), :] = res[pl.ds(2 * j + lax.bitwise_and(key, 1), 1), :]
            return carry

        lax.fori_loop(0, CHUNK // UNROLL, scatter, 0)
        return carry

    lax.fori_loop(0, n_chunks, body, 0)


def exchange_kernel(s_in, valid, target, probs, logp, pair_far, pair_own, far_send, far_recv, turned, scores,
                    pf_s, pf_r, po_s, po_r, x_s, x_r, t_s, t_r):
    me = lax.axis_index('vocab')
    core = lax.rem(me, 2)
    partner = me + 1 - 2 * core
    chip = lax.div(me, 2)
    far = me + 2 - 4 * chip
    length = valid.shape[1]
    half = length // 2
    part = half // PARTS
    rows = probs.shape[0]
    width = 2 * rows

    barrier = pltpu.get_barrier_semaphore()
    for peer in (partner, far):
        pl.semaphore_signal(barrier, inc=1, device_id={'vocab': peer}, device_id_type=MESH)
    pl.semaphore_wait(barrier, 2)

    def mine(q):
        return pl.ds(pl.multiple_of(core * half + q * part, part), part)

    def theirs(q):
        return pl.ds(pl.multiple_of((1 - core) * half + q * part, part), part)

    def remote(src, dst, s, r, peer):
        return pltpu.make_async_remote_copy(src_ref=src, dst_ref=dst, send_sem=s, recv_sem=r, device_id={'vocab': peer}, device_id_type=MESH)

    to_pair_far = [remote(s_in.at[theirs(q), pl.ds(width, width)], pair_far.at[q], pf_s.at[q], pf_r.at[q], partner) for q in range(PARTS)]
    to_pair_own = [remote(s_in.at[theirs(q), pl.ds(0, width)], pair_own.at[q], po_s.at[q], po_r.at[q], partner) for q in range(PARTS)]
    to_far = [remote(far_send.at[q], far_recv.at[q], x_s.at[q], x_r.at[q], far) for q in range(PARTS)]
    to_pair = [remote(turned.at[q, pl.ds(pl.multiple_of((1 - core) * rows, rows), rows)], scores.at[core, :, pl.ds(q * part, part)], t_s.at[q], t_r.at[q], partner) for q in range(PARTS)]
    for copy in to_pair_far + to_pair_own:
        copy.start()
    for q in range(PARTS):
        to_pair_far[q].wait_recv()
        far_send[q] = s_in[mine(q), width:] + pair_far[q]
        to_far[q].start()
    for q in range(PARTS):
        to_pair_own[q].wait_recv()
        pair_own[q] = s_in[mine(q), :width] + pair_own[q]
    for q in range(PARTS):
        to_far[q].wait_recv()
        turned[q] = (pair_own[q] + far_recv[q]).T * INV_TEMP
        to_pair[q].start()
        scores[core, :, q * part:(q + 1) * part] = turned[q, pl.ds(pl.multiple_of(core * rows, rows), rows)]
    for copy in to_pair:
        copy.wait_recv()

    s = jnp.concatenate([scores[0], scores[1]], axis=1)
    keep = jnp.broadcast_to(valid[...] > 0, s.shape)
    top = jnp.max(jnp.where(keep, s, -jnp.inf), axis=1, keepdims=True)
    total = jnp.sum(jnp.where(keep, jnp.exp(s - top), 0.0), axis=1, keepdims=True)
    log_norm = top + jnp.log(total)
    probs[...] = jnp.where(keep, jnp.exp(s - log_norm), 0.0)
    hit = lax.broadcasted_iota(jnp.int32, s.shape, 1) == target[...]
    logp[...] = jnp.sum(jnp.where(hit, s, 0.0), axis=1, keepdims=True) - log_norm
    for copy in to_pair_far + to_pair_own + to_far + to_pair:
        copy.wait_send()


def solution(mesh):
    shards = mesh.shape['vocab']
    across = [(i, i ^ 2) for i in range(shards)]
    beside = [(i, i ^ 1) for i in range(shards)]

    def device_step(hidden, w_head, allowed_ids, allowed_valid, target_pos):
        rows_dev, depth = hidden.shape
        vocab_local = w_head.shape[0]
        length = allowed_ids.shape[0]
        row_bits = vocab_local.bit_length() - 1
        width = rows_dev * shards
        ktiles = depth // LANES
        h_far = lax.ppermute(hidden, 'vocab', across)
        h_pair = lax.ppermute(hidden, 'vocab', beside)
        h_far_pair = lax.ppermute(h_far, 'vocab', beside)

        me = lax.axis_index('vocab')
        mine = (lax.shift_right_logical(allowed_ids, row_bits) == me) & (allowed_valid > 0)
        keys = jnp.where(mine, 0, length << row_bits) + (jnp.arange(length, dtype=jnp.int32) << row_bits) + lax.bitwise_and(allowed_ids, vocab_local - 1)
        keys = lax.sort(keys)
        count = jnp.sum(mine.astype(jnp.int32)).reshape(1)

        w_view = w_head.reshape(vocab_local // TILE_ROWS, TILE_ROWS, ktiles, LANES).transpose(0, 2, 1, 3).reshape(vocab_local // TILE_ROWS, ktiles, TILE_ROWS // 2, 2, LANES)
        any_spec = pl.BlockSpec(memory_space=pl.ANY)
        smem_spec = pl.BlockSpec(memory_space=pltpu.SMEM)
        vmem_spec = pl.BlockSpec(memory_space=pltpu.VMEM)
        own_scores = pl.pallas_call(
            functools.partial(gather_dot_kernel, row_bits=row_bits, trash=length),
            out_shape=jax.ShapeDtypeStruct((length + 8, width), jnp.float32),
            in_specs=[smem_spec, smem_spec] + [any_spec] * 5,
            out_specs=vmem_spec,
            scratch_shapes=[
                pltpu.VMEM((BUFS, ktiles, CHUNK, 2, LANES), jnp.bfloat16),
                pltpu.VMEM((width, depth), jnp.bfloat16),
                pltpu.VMEM((2 * CHUNK, width), jnp.float32),
                pltpu.SemaphoreType.DMA((4,)),
                pltpu.SemaphoreType.DMA((BUFS,)),
            ],
        )(keys, count, w_view, hidden, h_pair, h_far, h_far_pair)

        part = length // 2 // PARTS
        probs, logp = pl.pallas_call(
            exchange_kernel,
            out_shape=(jax.ShapeDtypeStruct((rows_dev, length), jnp.float32), jax.ShapeDtypeStruct((rows_dev, 1), jnp.float32)),
            in_specs=[vmem_spec] * 3,
            out_specs=(vmem_spec, vmem_spec),
            scratch_shapes=[pltpu.VMEM((PARTS, part, 2 * rows_dev), jnp.float32)] * 4
            + [pltpu.VMEM((PARTS, 2 * rows_dev, part), jnp.float32), pltpu.VMEM((2, rows_dev, length // 2), jnp.float32)]
            + [pltpu.SemaphoreType.DMA((PARTS,))] * 8,
            compiler_params=pltpu.CompilerParams(collective_id=0, has_side_effects=True),
        )(own_scores, allowed_valid.reshape(1, length), target_pos.reshape(rows_dev, 1))
        return probs, logp.reshape(rows_dev)

    row_spec = P(('rep', 'vocab'))
    mat_spec = P(('rep', 'vocab'), None)
    return jax.shard_map(device_step, mesh=mesh, in_specs=(mat_spec, P('vocab', None), P('rep'), P('rep'), row_spec), out_specs=(mat_spec, row_spec), check_vma=False)
```

```python
import functools

import jax
import jax.numpy as jnp
from jax import lax
from jax.experimental import pallas as pl
from jax.experimental.pallas import tpu as pltpu
from jax.sharding import PartitionSpec as P

INV_TEMP = 1.25
MESH = pl.DeviceIdType.MESH
LANES = 128
TILE_ROWS = 8
MIB = 1 << 20
CHUNK = 128
ISSUE = 8
PLACE = 32
PARTS = 4


def listed(keys, limit):
    length = keys.shape[0]
    low = jnp.int32(0)
    step = length
    while step:
        probe = low + step
        below = keys[jnp.minimum(probe, length) - 1] < limit
        low = jnp.where(below & (probe <= length), probe, low)
        step //= 2
    return low


def gather_kernel(keys, w, pairs, sem, *, row_bits):
    n_chunks = lax.div(listed(keys, keys.shape[0] << row_bits) + CHUNK - 1, CHUNK)

    def issue(i, carry):
        for u in range(ISSUE):
            j = i * ISSUE + u
            row = lax.bitwise_and(keys[j], (1 << row_bits) - 1)
            src = w.at[lax.shift_right_logical(row, 3), :, lax.bitwise_and(lax.shift_right_logical(row, 1), 3)]
            pltpu.make_async_copy(src, pairs.at[:, j], sem).start()
        return carry

    lax.fori_loop(0, n_chunks * (CHUNK // ISSUE), issue, 0)

    def wait(c, carry):
        chunk = pairs.at[:, pl.ds(0, CHUNK)]
        pltpu.make_async_copy(chunk, chunk, sem).wait()
        return carry

    lax.fori_loop(0, n_chunks, wait, 0)


def dot_kernel(keys, pos, pick, rows, h_own, h_pair, h_far, h_far_pair, near_out, far_out, hidden, res_near, res_far, *, row_bits):
    core = lax.rem(lax.axis_index('vocab'), 2)
    rows_dev = h_own.shape[0]
    length = keys.shape[0]
    ktiles = rows.shape[0]
    for src, which in ((h_own, core), (h_pair, 1 - core), (h_far, 2 + core), (h_far_pair, 3 - core)):
        hidden[pl.ds(pl.multiple_of(which * rows_dev, rows_dev), rows_dev), :] = src[...]

    def zero(i, carry):
        at = pl.ds(pl.multiple_of(i * 128, 128), 128)
        near_out[at, :] = jnp.zeros((128, LANES), jnp.float32)
        far_out[at, :] = jnp.zeros((128, LANES), jnp.float32)
        return carry

    lax.fori_loop(0, length // 128, zero, 0)

    def body(c, carry):
        at = pl.ds(pl.multiple_of(c * 2 * CHUNK, 2 * CHUNK), 2 * CHUNK)
        lhs = jnp.concatenate([rows[k, at] for k in range(ktiles)], axis=1)
        acc = lax.dot_general(lhs, hidden[...], (((1,), (1,)), ((), ())), preferred_element_type=jnp.float32)
        res_near[...] = acc[:, :LANES]
        res_far[...] = acc[:, LANES:]

        def place(i, carry):
            spots, near, far = [], [], []
            for u in range(PLACE):
                j = c * CHUNK + i * PLACE + u
                line = pl.ds(pick[j], 1)
                spots.append(pl.ds(pos[j], 1))
                near.append(res_near[line, :])
                far.append(res_far[line, :])
            for u in range(PLACE):
                near_out[spots[u], :] = near[u]
                far_out[spots[u], :] = far[u]
            return carry

        lax.fori_loop(0, CHUNK // PLACE, place, 0)
        return carry

    lax.fori_loop(0, lax.div(listed(keys, length << row_bits) + CHUNK - 1, CHUNK), body, 0)


def exchange_kernel(near_in, far_in, valid, target, probs, logp, pair_far, pair_own, far_send, far_recv, turned, scores,
                    pf_s, pf_r, po_s, po_r, x_s, x_r, t_s, t_r):
    me = lax.axis_index('vocab')
    core = lax.rem(me, 2)
    partner = me + 1 - 2 * core
    chip = lax.div(me, 2)
    far = me + 2 - 4 * chip
    length = valid.shape[1]
    half = length // 2
    part = half // PARTS
    rows = probs.shape[0]

    barrier = pltpu.get_barrier_semaphore()
    for peer in (partner, far):
        pl.semaphore_signal(barrier, inc=1, device_id={'vocab': peer}, device_id_type=MESH)
    pl.semaphore_wait(barrier, 2)

    def mine(q):
        return pl.ds(pl.multiple_of(core * half + q * part, part), part)

    def theirs(q):
        return pl.ds(pl.multiple_of((1 - core) * half + q * part, part), part)

    def remote(src, dst, s, r, peer):
        return pltpu.make_async_remote_copy(src_ref=src, dst_ref=dst, send_sem=s, recv_sem=r, device_id={'vocab': peer}, device_id_type=MESH)

    to_pair_far = [remote(far_in.at[theirs(q)], pair_far.at[q], pf_s.at[q], pf_r.at[q], partner) for q in range(PARTS)]
    to_pair_own = [remote(near_in.at[theirs(q)], pair_own.at[q], po_s.at[q], po_r.at[q], partner) for q in range(PARTS)]
    to_far = [remote(far_send.at[q], far_recv.at[q], x_s.at[q], x_r.at[q], far) for q in range(PARTS)]
    to_pair = [remote(turned.at[q, pl.ds(pl.multiple_of((1 - core) * rows, rows), rows)], scores.at[core, :, pl.ds(q * part, part)], t_s.at[q], t_r.at[q], partner) for q in range(PARTS)]
    for copy in to_pair_far + to_pair_own:
        copy.start()
    for q in range(PARTS):
        to_pair_far[q].wait_recv()
        far_send[q] = far_in[mine(q), :] + pair_far[q]
        to_far[q].start()
    for q in range(PARTS):
        to_pair_own[q].wait_recv()
        pair_own[q] = near_in[mine(q), :] + pair_own[q]
    for q in range(PARTS):
        to_far[q].wait_recv()
        turned[q] = (pair_own[q] + far_recv[q]).T * INV_TEMP
        to_pair[q].start()
        scores[core, :, q * part:(q + 1) * part] = turned[q, pl.ds(pl.multiple_of(core * rows, rows), rows)]
    for copy in to_pair:
        copy.wait_recv()

    s = jnp.concatenate([scores[0], scores[1]], axis=1)
    keep = jnp.broadcast_to(valid[...] > 0, s.shape)
    top = jnp.max(jnp.where(keep, s, -jnp.inf), axis=1, keepdims=True)
    total = jnp.sum(jnp.where(keep, jnp.exp(s - top), 0.0), axis=1, keepdims=True)
    log_norm = top + jnp.log(total)
    probs[...] = jnp.where(keep, jnp.exp(s - log_norm), 0.0)
    wanted = jnp.broadcast_to(target[...], (LANES, rows)).T[:, :1]
    hit = lax.broadcasted_iota(jnp.int32, s.shape, 1) == wanted
    picked = jnp.sum(jnp.where(hit, s, 0.0), axis=1, keepdims=True) - log_norm
    logp[...] = jnp.broadcast_to(picked, (rows, LANES)).T[:1, :]
    for copy in to_pair_far + to_pair_own + to_far + to_pair:
        copy.wait_send()


def solution(mesh):
    shards = mesh.shape['vocab']
    across = [(i, i ^ 2) for i in range(shards)]
    beside = [(i, i ^ 1) for i in range(shards)]

    def device_step(hidden, w_head, allowed_ids, allowed_valid, target_pos):
        rows_dev, depth = hidden.shape
        vocab_local = w_head.shape[0]
        length = allowed_ids.shape[0]
        row_bits = vocab_local.bit_length() - 1
        width = rows_dev * shards
        ktiles = depth // LANES
        h_far = lax.ppermute(hidden, 'vocab', across)
        h_pair = lax.ppermute(hidden, 'vocab', beside)

        me = lax.axis_index('vocab')
        mine = (lax.shift_right_logical(allowed_ids, row_bits) == me) & (allowed_valid > 0)
        places = jnp.arange(length, dtype=jnp.int32)
        keys = lax.sort(jnp.where(mine, places, places + length) * vocab_local + lax.bitwise_and(allowed_ids, vocab_local - 1))
        pos = jnp.minimum(lax.shift_right_logical(keys, row_bits), length)
        pick = 2 * lax.rem(places, CHUNK) + lax.bitwise_and(keys, 1)

        target = target_pos.reshape(1, rows_dev)
        keys, pos, pick, target, h_pair = lax.optimization_barrier((keys, pos, pick, target, h_pair))

        w_view = w_head.reshape(vocab_local // TILE_ROWS, TILE_ROWS, ktiles, LANES).transpose(0, 2, 1, 3).reshape(vocab_local // TILE_ROWS, ktiles, TILE_ROWS // 2, 2, LANES)
        any_spec = pl.BlockSpec(memory_space=pl.ANY)
        smem_spec = pl.BlockSpec(memory_space=pltpu.SMEM)
        vmem_spec = pl.BlockSpec(memory_space=pltpu.VMEM)
        pairs = pl.pallas_call(
            functools.partial(gather_kernel, row_bits=row_bits),
            out_shape=pltpu.VMEM((ktiles, length, 2, LANES), jnp.bfloat16),
            in_specs=[smem_spec, any_spec],
            out_specs=vmem_spec,
            scratch_shapes=[pltpu.SemaphoreType.DMA],
            compiler_params=pltpu.CompilerParams(vmem_limit_bytes=2 * MIB),
        )(keys, w_view)
        h_far, pairs = lax.optimization_barrier((h_far, pairs))
        h_far_pair = lax.ppermute(h_far, 'vocab', beside)
        pair_rows = pltpu.with_memory_space_constraint(pairs.reshape(ktiles, 2 * length, LANES), pltpu.VMEM)
        near, far = pl.pallas_call(
            functools.partial(dot_kernel, row_bits=row_bits),
            out_shape=(pltpu.VMEM((length + 8, LANES), jnp.float32), pltpu.VMEM((length + 8, LANES), jnp.float32)),
            in_specs=[smem_spec] * 3 + [vmem_spec] * 5,
            out_specs=(vmem_spec, vmem_spec),
            scratch_shapes=[
                pltpu.VMEM((width, depth), jnp.bfloat16),
                pltpu.VMEM((2 * CHUNK, LANES), jnp.float32),
                pltpu.VMEM((2 * CHUNK, LANES), jnp.float32),
            ],
            compiler_params=pltpu.CompilerParams(vmem_limit_bytes=9 * MIB),
        )(keys, pos, pick, pair_rows, hidden, h_pair, h_far, h_far_pair)

        part = length // 2 // PARTS
        near = pltpu.with_memory_space_constraint(near, pltpu.VMEM)
        far = pltpu.with_memory_space_constraint(far, pltpu.VMEM)
        probs, logp = pl.pallas_call(
            exchange_kernel,
            out_shape=(pltpu.VMEM((rows_dev, length), jnp.float32), jax.ShapeDtypeStruct((1, rows_dev), jnp.float32)),
            in_specs=[vmem_spec] * 4,
            out_specs=(vmem_spec, vmem_spec),
            scratch_shapes=[pltpu.VMEM((PARTS, part, 2 * rows_dev), jnp.float32)] * 4
            + [pltpu.VMEM((PARTS, 2 * rows_dev, part), jnp.float32), pltpu.VMEM((2, rows_dev, length // 2), jnp.float32)]
            + [pltpu.SemaphoreType.DMA((PARTS,))] * 8,
            compiler_params=pltpu.CompilerParams(collective_id=0, has_side_effects=True, vmem_limit_bytes=24 * MIB),
        )(near, far, allowed_valid.reshape(1, length), target)
        return probs, logp.reshape(rows_dev)

    row_spec = P(('rep', 'vocab'))
    mat_spec = P(('rep', 'vocab'), None)
    return jax.shard_map(device_step, mesh=mesh, in_specs=(mat_spec, P('vocab', None), P('rep'), P('rep'), row_spec), out_specs=(mat_spec, row_spec), check_vma=False)
```

```python
import functools

import jax
import jax.numpy as jnp
from jax import lax
from jax.experimental import pallas as pl
from jax.experimental.pallas import tpu as pltpu
from jax.sharding import PartitionSpec as P

INV_TEMP = 1.25
MESH = pl.DeviceIdType.MESH
LANES = 128
TILE_ROWS = 8
MIB = 1 << 20
ISSUE = 8
PARTS = 4


def listed(keys, limit):
    length = keys.shape[0]
    low = jnp.int32(0)
    step = length
    while step:
        probe = low + step
        below = keys[jnp.minimum(probe, length) - 1] < limit
        low = jnp.where(below & (probe <= length), probe, low)
        step //= 2
    return low


def gather_kernel(keys, w, pairs, sem, *, row_bits):
    length = keys.shape[0]
    n_groups = lax.div(listed(keys, length << row_bits) + ISSUE - 1, ISSUE)

    def issue(i, carry):
        for u in range(ISSUE):
            key = keys[i * ISSUE + u]
            row = lax.bitwise_and(key, (1 << row_bits) - 1)
            src = w.at[lax.shift_right_logical(row, 3), :, lax.bitwise_and(lax.shift_right_logical(row, 1), 3)]
            spot = lax.bitwise_and(lax.shift_right_logical(key, row_bits), length - 1)
            pltpu.make_async_copy(src, pairs.at[:, spot], sem).start()
        return carry

    lax.fori_loop(0, n_groups, issue, 0)

    def wait(i, carry):
        group = pairs.at[:, pl.ds(0, ISSUE)]
        pltpu.make_async_copy(group, group, sem).wait()
        return carry

    lax.fori_loop(0, n_groups, wait, 0)


def score_kernel(code, rows, h_own, h_pair, h_far, h_far_pair, valid, target, probs, logp, hidden, both, give_near, give_far,
                 pair_near, pair_far, near, far_send, far_recv, turned, scores, gf_s, gf_r, gn_s, gn_r, x_s, x_r, t_s, t_r):
    me = lax.axis_index('vocab')
    core = lax.rem(me, 2)
    partner = me + 1 - 2 * core
    far = me + 2 - 4 * lax.div(me, 2)
    length = valid.shape[1]
    half = length // 2
    part = half // PARTS
    rows_dev = probs.shape[0]
    ktiles = rows.shape[0]

    barrier = pltpu.get_barrier_semaphore()
    for peer in (partner, far):
        pl.semaphore_signal(barrier, inc=1, device_id={'vocab': peer}, device_id_type=MESH)
    for src, which in ((h_own, core), (h_pair, 1 - core), (h_far, 2 + core), (h_far_pair, 3 - core)):
        hidden[pl.ds(pl.multiple_of(which * rows_dev, rows_dev), rows_dev), :] = src[...]
    pl.semaphore_wait(barrier, 2)

    def remote(src, dst, s, r, peer):
        return pltpu.make_async_remote_copy(src_ref=src, dst_ref=dst, send_sem=s, recv_sem=r, device_id={'vocab': peer}, device_id_type=MESH)

    def give_far_copy(q):
        return remote(give_far.at[q], pair_far.at[q], gf_s.at[q], gf_r.at[q], partner)

    def give_near_copy(q):
        return remote(give_near.at[q], pair_near.at[q], gn_s.at[q], gn_r.at[q], partner)

    def far_copy(q):
        return remote(far_send.at[q], far_recv.at[q], x_s.at[q], x_r.at[q], far)

    def turn_copy(q):
        src = turned.at[q, pl.ds(pl.multiple_of((1 - core) * rows_dev, rows_dev), rows_dev)]
        return remote(src, scores.at[core, :, pl.ds(pl.multiple_of(q * part, part), part)], t_s.at[q], t_r.at[q], partner)

    def part_scores(start):
        at = pl.ds(pl.multiple_of(2 * start, 2 * part), 2 * part)
        acc = jnp.zeros((2 * part, 2 * LANES), jnp.float32)
        for k in range(0, ktiles, 2):
            lhs = jnp.concatenate([rows[k, at], rows[k + 1, at]], axis=1)
            acc += lax.dot_general(lhs, hidden[:, k * LANES:(k + 2) * LANES], (((1,), (1,)), ((), ())), preferred_element_type=jnp.float32)
        both[0] = acc[:, :LANES]
        both[1] = acc[:, LANES:]
        kind = jnp.broadcast_to(code[:, pl.ds(pl.multiple_of(start, part), part)], (LANES, part)).T
        picked = []
        for side in range(2):
            even = both[side, pl.ds(0, part, 2), :]
            odd = both[side, pl.ds(1, part, 2), :]
            picked.append(jnp.where(kind == 2, odd, jnp.where(kind == 1, even, 0.0)))
        return picked

    def step(q, carry):
        near_part, far_part = part_scores((1 - core) * half + q * part)
        give_far[q] = far_part
        give_far_copy(q).start()
        give_near[q] = near_part
        give_near_copy(q).start()
        near_part, far_part = part_scores(core * half + q * part)
        give_far_copy(q).wait_recv()
        far_send[q] = far_part + pair_far[q]
        far_copy(q).start()
        give_near_copy(q).wait_recv()
        near[q] = near_part + pair_near[q]
        return carry

    lax.fori_loop(0, PARTS, step, 0)
    for q in range(PARTS):
        far_copy(q).wait_recv()
        turned[q] = (near[q] + far_recv[q]).T * INV_TEMP
        turn_copy(q).start()
        scores[core, :, q * part:(q + 1) * part] = turned[q, pl.ds(pl.multiple_of(core * rows_dev, rows_dev), rows_dev)]
    for q in range(PARTS):
        turn_copy(q).wait_recv()

    s = jnp.concatenate([scores[0], scores[1]], axis=1)
    keep = jnp.broadcast_to(valid[...] > 0, s.shape)
    top = jnp.max(jnp.where(keep, s, -jnp.inf), axis=1, keepdims=True)
    total = jnp.sum(jnp.where(keep, jnp.exp(s - top), 0.0), axis=1, keepdims=True)
    log_norm = top + jnp.log(total)
    probs[...] = jnp.where(keep, jnp.exp(s - log_norm), 0.0)
    wanted = jnp.broadcast_to(target[...], (LANES, rows_dev)).T[:, :1]
    hit = lax.broadcasted_iota(jnp.int32, s.shape, 1) == wanted
    picked = jnp.sum(jnp.where(hit, s, 0.0), axis=1, keepdims=True) - log_norm
    logp[...] = jnp.broadcast_to(picked, (rows_dev, LANES)).T[:1, :]
    for q in range(PARTS):
        give_far_copy(q).wait_send()
        give_near_copy(q).wait_send()
        far_copy(q).wait_send()
        turn_copy(q).wait_send()


def solution(mesh):
    shards = mesh.shape['vocab']
    across = [(i, i ^ 2) for i in range(shards)]
    beside = [(i, i ^ 1) for i in range(shards)]

    def device_step(hidden, w_head, allowed_ids, allowed_valid, target_pos):
        rows_dev, depth = hidden.shape
        vocab_local = w_head.shape[0]
        length = allowed_ids.shape[0]
        row_bits = vocab_local.bit_length() - 1
        width = rows_dev * shards
        ktiles = depth // LANES
        h_far = lax.ppermute(hidden, 'vocab', across)
        h_pair = lax.ppermute(hidden, 'vocab', beside)

        me = lax.axis_index('vocab')
        mine = (lax.shift_right_logical(allowed_ids, row_bits) == me) & (allowed_valid > 0)
        places = jnp.arange(length, dtype=jnp.int32)
        keys = lax.sort(jnp.where(mine, places, places + length) * vocab_local + lax.bitwise_and(allowed_ids, vocab_local - 1))
        code = jnp.where(mine, 1 + lax.bitwise_and(allowed_ids, 1), 0).reshape(1, length)

        target = target_pos.reshape(1, rows_dev)
        keys, code, target, h_pair = lax.optimization_barrier((keys, code, target, h_pair))

        w_view = w_head.reshape(vocab_local // TILE_ROWS, TILE_ROWS, ktiles, LANES).transpose(0, 2, 1, 3).reshape(vocab_local // TILE_ROWS, ktiles, TILE_ROWS // 2, 2, LANES)
        any_spec = pl.BlockSpec(memory_space=pl.ANY)
        smem_spec = pl.BlockSpec(memory_space=pltpu.SMEM)
        vmem_spec = pl.BlockSpec(memory_space=pltpu.VMEM)
        pairs = pl.pallas_call(
            functools.partial(gather_kernel, row_bits=row_bits),
            out_shape=pltpu.VMEM((ktiles, length, 2, LANES), jnp.bfloat16),
            in_specs=[smem_spec, any_spec],
            out_specs=vmem_spec,
            scratch_shapes=[pltpu.SemaphoreType.DMA],
            compiler_params=pltpu.CompilerParams(vmem_limit_bytes=2 * MIB),
        )(keys, w_view)
        h_far, pairs = lax.optimization_barrier((h_far, pairs))
        h_far_pair = lax.ppermute(h_far, 'vocab', beside)
        pair_rows = pltpu.with_memory_space_constraint(pairs.reshape(ktiles, 2 * length, LANES), pltpu.VMEM)
        part = length // 2 // PARTS
        probs, logp = pl.pallas_call(
            score_kernel,
            out_shape=(pltpu.VMEM((rows_dev, length), jnp.float32), jax.ShapeDtypeStruct((1, rows_dev), jnp.float32)),
            in_specs=[vmem_spec] * 8,
            out_specs=(vmem_spec, vmem_spec),
            scratch_shapes=[pltpu.VMEM((width, depth), jnp.bfloat16), pltpu.VMEM((2, 2 * part, LANES), jnp.float32)]
            + [pltpu.VMEM((PARTS, part, LANES), jnp.float32)] * 7
            + [pltpu.VMEM((PARTS, LANES, part), jnp.float32), pltpu.VMEM((2, rows_dev, length // 2), jnp.float32)]
            + [pltpu.SemaphoreType.DMA((PARTS,))] * 8,
            compiler_params=pltpu.CompilerParams(collective_id=0, has_side_effects=True, vmem_limit_bytes=10 * MIB),
        )(code, pair_rows, hidden, h_pair, h_far, h_far_pair, allowed_valid.reshape(1, length), target)
        return probs, logp.reshape(rows_dev)

    row_spec = P(('rep', 'vocab'))
    mat_spec = P(('rep', 'vocab'), None)
    return jax.shard_map(device_step, mesh=mesh, in_specs=(mat_spec, P('vocab', None), P('rep'), P('rep'), row_spec), out_specs=(mat_spec, row_spec), check_vma=False)
```

```python
import functools

import jax
import jax.numpy as jnp
from jax import lax
from jax.experimental import pallas as pl
from jax.experimental.pallas import tpu as pltpu
from jax.sharding import PartitionSpec as P

INV_TEMP = 1.25
MESH = pl.DeviceIdType.MESH
LANES = 128
TILE_ROWS = 8
MIB = 1 << 20
ISSUE = 8
PARTS = 4


def listed(keys, limit):
    length = keys.shape[0]
    low = jnp.int32(0)
    step = length
    while step:
        probe = low + step
        below = keys[jnp.minimum(probe, length) - 1] < limit
        low = jnp.where(below & (probe <= length), probe, low)
        step //= 2
    return low


def gather_kernel(keys, w, pairs, sem, *, row_bits):
    length = keys.shape[0]
    n_groups = lax.div(listed(keys, length << row_bits) + ISSUE - 1, ISSUE)

    def issue(i, carry):
        for u in range(ISSUE):
            key = keys[i * ISSUE + u]
            row = lax.bitwise_and(key, (1 << row_bits) - 1)
            src = w.at[lax.shift_right_logical(row, 3), :, lax.bitwise_and(lax.shift_right_logical(row, 1), 3)]
            spot = lax.bitwise_and(lax.shift_right_logical(key, row_bits), length - 1)
            pltpu.make_async_copy(src, pairs.at[:, spot], sem).start()
        return carry

    lax.fori_loop(0, n_groups, issue, 0)

    def wait(i, carry):
        group = pairs.at[:, pl.ds(0, ISSUE)]
        pltpu.make_async_copy(group, group, sem).wait()
        return carry

    lax.fori_loop(0, n_groups, wait, 0)


def score_kernel(code, rows, h_own, h_pair, h_far, h_far_pair, valid, target, probs, logp, hidden, both, give_near, give_far,
                 pair_near, pair_far, near, far_send, far_recv, turned, scores, gf_s, gf_r, gn_s, gn_r, x_s, x_r, t_s, t_r):
    me = lax.axis_index('vocab')
    core = lax.rem(me, 2)
    partner = me + 1 - 2 * core
    far = me + 2 - 4 * lax.div(me, 2)
    length = valid.shape[1]
    half = length // 2
    part = half // PARTS
    rows_dev = probs.shape[0]
    ktiles = rows.shape[0]

    barrier = pltpu.get_barrier_semaphore()
    for peer in (partner, far):
        pl.semaphore_signal(barrier, inc=1, device_id={'vocab': peer}, device_id_type=MESH)
    for src, which in ((h_own, core), (h_pair, 1 - core), (h_far, 2 + core), (h_far_pair, 3 - core)):
        hidden[pl.ds(pl.multiple_of(which * rows_dev, rows_dev), rows_dev), :] = src[...]
    pl.semaphore_wait(barrier, 2)

    def remote(src, dst, s, r, peer):
        return pltpu.make_async_remote_copy(src_ref=src, dst_ref=dst, send_sem=s, recv_sem=r, device_id={'vocab': peer}, device_id_type=MESH)

    def give_far_copy(q):
        return remote(give_far.at[q], pair_far.at[q], gf_s.at[q], gf_r.at[q], partner)

    def give_near_copy(q):
        return remote(give_near.at[q], pair_near.at[q], gn_s.at[q], gn_r.at[q], partner)

    def far_copy(q):
        return remote(far_send.at[q], far_recv.at[q], x_s.at[q], x_r.at[q], far)

    def turn_copy(q):
        src = turned.at[q, pl.ds(pl.multiple_of((1 - core) * rows_dev, rows_dev), rows_dev)]
        return remote(src, scores.at[core, :, pl.ds(pl.multiple_of(q * part, part), part)], t_s.at[q], t_r.at[q], partner)

    def part_scores(start):
        at = pl.ds(pl.multiple_of(2 * start, 2 * part), 2 * part)
        for t in range(2 * part // 256):
            at = pl.ds(pl.multiple_of(2 * start + t * 256, 256), 256)
            acc = jnp.zeros((256, 2 * LANES), jnp.float32)
            for k in range(0, ktiles, 2):
                lhs = jnp.concatenate([rows[k, at], rows[k + 1, at]], axis=1)
                acc += lax.dot_general(lhs, hidden[:, k * LANES:(k + 2) * LANES], (((1,), (1,)), ((), ())), preferred_element_type=jnp.float32)
            both[0, t * 256:(t + 1) * 256] = acc[:, :LANES]
            both[1, t * 256:(t + 1) * 256] = acc[:, LANES:]
        kind = jnp.broadcast_to(code[:, pl.ds(pl.multiple_of(start, part), part)], (LANES, part)).T
        picked = []
        for side in range(2):
            even = both[side, pl.ds(0, part, 2), :]
            odd = both[side, pl.ds(1, part, 2), :]
            picked.append(jnp.where(kind == 2, odd, jnp.where(kind == 1, even, 0.0)))
        return picked

    def step(q, carry):
        near_part, far_part = part_scores((1 - core) * half + q * part)
        give_far[q] = far_part
        give_far_copy(q).start()
        give_near[q] = near_part
        give_near_copy(q).start()
        near_part, far_part = part_scores(core * half + q * part)
        give_far_copy(q).wait_recv()
        far_send[q] = far_part + pair_far[q]
        far_copy(q).start()
        give_near_copy(q).wait_recv()
        near[q] = near_part + pair_near[q]
        return carry

    lax.fori_loop(0, PARTS, step, 0)
    for q in range(PARTS):
        far_copy(q).wait_recv()
        turned[q] = (near[q] + far_recv[q]).T * INV_TEMP
        turn_copy(q).start()
        scores[core, :, q * part:(q + 1) * part] = turned[q, pl.ds(pl.multiple_of(core * rows_dev, rows_dev), rows_dev)]
    for q in range(PARTS):
        turn_copy(q).wait_recv()

    s = jnp.concatenate([scores[0], scores[1]], axis=1)
    keep = jnp.broadcast_to(valid[...] > 0, s.shape)
    top = jnp.max(jnp.where(keep, s, -jnp.inf), axis=1, keepdims=True)
    total = jnp.sum(jnp.where(keep, jnp.exp(s - top), 0.0), axis=1, keepdims=True)
    log_norm = top + jnp.log(total)
    probs[...] = jnp.where(keep, jnp.exp(s - log_norm), 0.0)
    wanted = jnp.broadcast_to(target[...], (LANES, rows_dev)).T[:, :1]
    hit = lax.broadcasted_iota(jnp.int32, s.shape, 1) == wanted
    picked = jnp.sum(jnp.where(hit, s, 0.0), axis=1, keepdims=True) - log_norm
    logp[...] = jnp.broadcast_to(picked, (rows_dev, LANES)).T[:1, :]
    for q in range(PARTS):
        give_far_copy(q).wait_send()
        give_near_copy(q).wait_send()
        far_copy(q).wait_send()
        turn_copy(q).wait_send()


def solution(mesh):
    shards = mesh.shape['vocab']
    across = [(i, i ^ 2) for i in range(shards)]
    beside = [(i, i ^ 1) for i in range(shards)]

    def device_step(hidden, w_head, allowed_ids, allowed_valid, target_pos):
        rows_dev, depth = hidden.shape
        vocab_local = w_head.shape[0]
        length = allowed_ids.shape[0]
        row_bits = vocab_local.bit_length() - 1
        width = rows_dev * shards
        ktiles = depth // LANES
        h_far = lax.ppermute(hidden, 'vocab', across)
        h_pair = lax.ppermute(hidden, 'vocab', beside)

        me = lax.axis_index('vocab')
        mine = (lax.shift_right_logical(allowed_ids, row_bits) == me) & (allowed_valid > 0)
        places = jnp.arange(length, dtype=jnp.int32)
        keys = lax.sort(jnp.where(mine, places, places + length) * vocab_local + lax.bitwise_and(allowed_ids, vocab_local - 1))
        code = jnp.where(mine, 1 + lax.bitwise_and(allowed_ids, 1), 0).reshape(1, length)

        target = target_pos.reshape(1, rows_dev)
        keys, code, target, h_pair = lax.optimization_barrier((keys, code, target, h_pair))

        w_view = w_head.reshape(vocab_local // TILE_ROWS, TILE_ROWS, ktiles, LANES).transpose(0, 2, 1, 3).reshape(vocab_local // TILE_ROWS, ktiles, TILE_ROWS // 2, 2, LANES)
        any_spec = pl.BlockSpec(memory_space=pl.ANY)
        smem_spec = pl.BlockSpec(memory_space=pltpu.SMEM)
        vmem_spec = pl.BlockSpec(memory_space=pltpu.VMEM)
        pairs = pl.pallas_call(
            functools.partial(gather_kernel, row_bits=row_bits),
            out_shape=pltpu.VMEM((ktiles, length, 2, LANES), jnp.bfloat16),
            in_specs=[smem_spec, any_spec],
            out_specs=vmem_spec,
            scratch_shapes=[pltpu.SemaphoreType.DMA],
            compiler_params=pltpu.CompilerParams(vmem_limit_bytes=2 * MIB),
        )(keys, w_view)
        h_far, pairs = lax.optimization_barrier((h_far, pairs))
        h_far_pair = lax.ppermute(h_far, 'vocab', beside)
        pair_rows = pltpu.with_memory_space_constraint(pairs.reshape(ktiles, 2 * length, LANES), pltpu.VMEM)
        part = length // 2 // PARTS
        probs, logp = pl.pallas_call(
            score_kernel,
            out_shape=(pltpu.VMEM((rows_dev, length), jnp.float32), jax.ShapeDtypeStruct((1, rows_dev), jnp.float32)),
            in_specs=[vmem_spec] * 8,
            out_specs=(vmem_spec, vmem_spec),
            scratch_shapes=[pltpu.VMEM((width, depth), jnp.bfloat16), pltpu.VMEM((2, 2 * part, LANES), jnp.float32)]
            + [pltpu.VMEM((PARTS, part, LANES), jnp.float32)] * 7
            + [pltpu.VMEM((PARTS, LANES, part), jnp.float32), pltpu.VMEM((2, rows_dev, length // 2), jnp.float32)]
            + [pltpu.SemaphoreType.DMA((PARTS,))] * 8,
            compiler_params=pltpu.CompilerParams(collective_id=0, has_side_effects=True, vmem_limit_bytes=10 * MIB),
        )(code, pair_rows, hidden, h_pair, h_far, h_far_pair, allowed_valid.reshape(1, length), target)
        return probs, logp.reshape(rows_dev)

    row_spec = P(('rep', 'vocab'))
    mat_spec = P(('rep', 'vocab'), None)
    return jax.shard_map(device_step, mesh=mesh, in_specs=(mat_spec, P('vocab', None), P('rep'), P('rep'), row_spec), out_specs=(mat_spec, row_spec), check_vma=False)
```

```python
import functools

import jax
import jax.numpy as jnp
from jax import lax
from jax.experimental import pallas as pl
from jax.experimental.pallas import tpu as pltpu
from jax.sharding import PartitionSpec as P

INV_TEMP = 1.25
MESH = pl.DeviceIdType.MESH
LANES = 128
TILE_ROWS = 8
MIB = 1 << 20
ISSUE = 8
PARTS = 8
BLOCK = 256
BAND = 16


def listed(keys, limit):
    length = keys.shape[0]
    low = jnp.int32(0)
    step = length
    while step:
        probe = low + step
        below = keys[jnp.minimum(probe, length) - 1] < limit
        low = jnp.where(below & (probe <= length), probe, low)
        step //= 2
    return low


def gather_kernel(keys, w, pairs, sem, *, row_bits):
    length = keys.shape[0]
    n_groups = lax.div(listed(keys, length << row_bits) + ISSUE - 1, ISSUE)

    def issue(i, carry):
        for u in range(ISSUE):
            key = keys[i * ISSUE + u]
            row = lax.bitwise_and(key, (1 << row_bits) - 1)
            src = w.at[lax.shift_right_logical(row, 3), :, lax.bitwise_and(lax.shift_right_logical(row, 1), 3)]
            spot = lax.bitwise_and(lax.shift_right_logical(key, row_bits), length - 1)
            pltpu.make_async_copy(src, pairs.at[:, spot], sem).start()
        return carry

    lax.fori_loop(0, n_groups, issue, 0)

    def wait(i, carry):
        group = pairs.at[:, pl.ds(0, ISSUE)]
        pltpu.make_async_copy(group, group, sem).wait()
        return carry

    lax.fori_loop(0, n_groups, wait, 0)


def block_dot(rows, at, blocks, first_tile):
    acc = jnp.zeros((BLOCK, sum(block.shape[0] for block in blocks)), jnp.float32)
    for k in range(0, blocks[0].shape[1] // LANES, 2):
        lhs = jnp.concatenate([rows[first_tile + k, at], rows[first_tile + k + 1, at]], axis=1)
        rhs = jnp.concatenate([block[:, k * LANES:(k + 2) * LANES] for block in blocks], axis=0)
        acc += lax.dot_general(lhs, rhs, (((1,), (1,)), ((), ())), preferred_element_type=jnp.float32)
    return acc


def score_kernel(ids, valid, target, rows, h_own, h_pair, h_far, h_far_pair, scores, norm, logp, both,
                 give, got, far_own, far_send, far_recv, g_s, g_r, x_s, x_r, *, row_bits):
    me = lax.axis_index('vocab')
    partner = me + 1 - 2 * lax.rem(me, 2)
    far = me + 2 - 4 * lax.div(me, 2)
    length = valid.shape[1]
    part = length // PARTS
    rows_dev = norm.shape[0]

    barrier = pltpu.get_barrier_semaphore()
    for peer in (partner, far):
        pl.semaphore_signal(barrier, inc=1, device_id={'vocab': peer}, device_id_type=MESH)

    def give_copy(p):
        return pltpu.make_async_remote_copy(src_ref=give.at[p], dst_ref=got.at[p], send_sem=g_s.at[p], recv_sem=g_r.at[p],
                                            device_id={'vocab': partner}, device_id_type=MESH)

    def far_copy(p):
        return pltpu.make_async_remote_copy(src_ref=far_send.at[p], dst_ref=far_recv.at[p], send_sem=x_s.at[p], recv_sem=x_r.at[p],
                                            device_id={'vocab': far}, device_id_type=MESH)

    def compute(p):
        for t in range(2 * part // BLOCK):
            at = pl.ds(pl.multiple_of(p * 2 * part + t * BLOCK, BLOCK), BLOCK)
            here = pl.ds(t * BLOCK, BLOCK)
            acc = block_dot(rows, at, (h_own, h_pair, h_far, h_far_pair), 0)
            both[0, here] = acc[:, :LANES]
            both[1, here] = acc[:, LANES:]
        spots = pl.ds(pl.multiple_of(p * part, part), part)
        ids_part = ids[:, spots]
        kind = jnp.where((lax.shift_right_logical(ids_part, row_bits) == me) & (valid[:, spots] > 0), 1 + lax.bitwise_and(ids_part, 1), 0)
        kind = jnp.broadcast_to(kind, (LANES, part)).T
        flat = []
        for side in range(2):
            even = both[side, pl.ds(0, part, 2), :]
            odd = both[side, pl.ds(1, part, 2), :]
            flat.append(jnp.where(kind == 2, odd, jnp.where(kind == 1, even, 0.0)).T)
        scores[p] = flat[0][:rows_dev]
        far_own[p] = flat[1][:rows_dev]
        give[p, 0] = flat[0][rows_dev:]
        give[p, 1] = flat[1][rows_dev:]

    def merge(p):
        give_copy(p).wait_recv()
        far_send[p] = far_own[p] + got[p, 1]
        far_copy(p).start()
        scores[p] = scores[p] + got[p, 0]

    compute(0)
    pl.semaphore_wait(barrier, 2)
    give_copy(0).start()

    def step(p, carry):
        compute(p)
        give_copy(p).start()
        merge(p - 1)
        return carry

    lax.fori_loop(1, PARTS, step, 0)
    merge(PARTS - 1)
    wanted = jnp.broadcast_to(target[...], (LANES, rows_dev)).T
    wanted = jnp.concatenate([wanted] * (part // LANES), axis=1)
    place = lax.broadcasted_iota(jnp.int32, (rows_dev, part), 1)
    top = jnp.full((rows_dev, part), -jnp.inf, jnp.float32)
    picked = jnp.zeros((rows_dev, part), jnp.float32)
    for p in range(PARTS):
        far_copy(p).wait_recv()
        s = (scores[p] + far_recv[p]) * INV_TEMP
        picked += jnp.where(place + p * part == wanted, s, 0.0)
        s = jnp.where(valid[:, p * part:(p + 1) * part] > 0, s, -jnp.inf)
        scores[p] = s
        top = jnp.maximum(top, s)
    top = jnp.max(top, axis=1, keepdims=True)
    total = jnp.zeros((rows_dev, part), jnp.float32)
    for p in range(PARTS):
        total += jnp.exp(scores[p] - top)
    log_norm = top + jnp.log(jnp.sum(total, axis=1, keepdims=True))
    norm[...] = jnp.broadcast_to(log_norm, (rows_dev, LANES))
    picked = jnp.sum(picked, axis=1, keepdims=True) - log_norm
    logp[...] = jnp.broadcast_to(picked, (rows_dev, LANES)).T[:1, :]
    for p in range(PARTS):
        give_copy(p).wait_send()
        far_copy(p).wait_send()


def finish_kernel(scores, norm, logp, probs_out, logp_out, probs, sem):
    parts, _, part = scores.shape
    bands = probs.shape[0] // BAND
    small = pltpu.make_async_copy(logp, logp_out, sem.at[bands])
    small.start()
    copies = []
    for band in range(bands):
        here = pl.ds(band * BAND, BAND)
        shift = jnp.concatenate([norm[here, :]] * (part // LANES), axis=1)
        for p in range(parts):
            probs[here, p * part:(p + 1) * part] = jnp.exp(scores[p, here] - shift)
        copies.append(pltpu.make_async_copy(probs.at[here], probs_out.at[here], sem.at[band]))
        copies[-1].start()
    for copy in copies:
        copy.wait()
    small.wait()


def solution(mesh):
    shards = mesh.shape['vocab']
    across = [(i, i ^ 2) for i in range(shards)]
    beside = [(i, i ^ 1) for i in range(shards)]

    def device_step(hidden, w_head, allowed_ids, allowed_valid, target_pos):
        rows_dev, depth = hidden.shape
        vocab_local = w_head.shape[0]
        length = allowed_ids.shape[0]
        row_bits = vocab_local.bit_length() - 1
        ktiles = depth // LANES
        h_far = lax.ppermute(hidden, 'vocab', across)
        me = lax.axis_index('vocab')
        mine = (lax.shift_right_logical(allowed_ids, row_bits) == me) & (allowed_valid > 0)
        places = jnp.arange(length, dtype=jnp.int32)
        keys = lax.sort(jnp.where(mine, places, places + length) * vocab_local + lax.bitwise_and(allowed_ids, vocab_local - 1))
        keys, hidden_again = lax.optimization_barrier((keys, hidden))
        h_pair = lax.ppermute(hidden_again, 'vocab', beside)

        w_view = w_head.reshape(vocab_local // TILE_ROWS, TILE_ROWS, ktiles, LANES).transpose(0, 2, 1, 3).reshape(vocab_local // TILE_ROWS, ktiles, TILE_ROWS // 2, 2, LANES)
        any_spec = pl.BlockSpec(memory_space=pl.ANY)
        smem_spec = pl.BlockSpec(memory_space=pltpu.SMEM)
        vmem_spec = pl.BlockSpec(memory_space=pltpu.VMEM)
        pairs = pl.pallas_call(
            functools.partial(gather_kernel, row_bits=row_bits),
            out_shape=pltpu.VMEM((ktiles, length, 2, LANES), jnp.bfloat16),
            in_specs=[smem_spec, any_spec],
            out_specs=vmem_spec,
            scratch_shapes=[pltpu.SemaphoreType.DMA],
            compiler_params=pltpu.CompilerParams(vmem_limit_bytes=2 * MIB),
        )(keys, w_view)
        h_far, pairs = lax.optimization_barrier((h_far, pairs))
        h_far_pair = lax.ppermute(h_far, 'vocab', beside)
        pair_rows = pltpu.with_memory_space_constraint(pairs.reshape(ktiles, 2 * length, LANES), pltpu.VMEM)
        part = length // PARTS
        masked, norm, logp = pl.pallas_call(
            functools.partial(score_kernel, row_bits=row_bits),
            out_shape=(pltpu.VMEM((PARTS, rows_dev, part), jnp.float32), pltpu.VMEM((rows_dev, LANES), jnp.float32), pltpu.VMEM((1, rows_dev), jnp.float32)),
            in_specs=[vmem_spec] * 8,
            out_specs=(vmem_spec,) * 3,
            scratch_shapes=[pltpu.VMEM((2, 2 * part, LANES), jnp.float32)]
            + [pltpu.VMEM((PARTS, 2, rows_dev, part), jnp.float32)] * 2
            + [pltpu.VMEM((PARTS, rows_dev, part), jnp.float32)] * 3
            + [pltpu.SemaphoreType.DMA((PARTS,))] * 4,
            compiler_params=pltpu.CompilerParams(collective_id=0, has_side_effects=True, vmem_limit_bytes=8 * MIB),
        )(allowed_ids.reshape(1, length), allowed_valid.reshape(1, length), target_pos.reshape(1, rows_dev), pair_rows, hidden, h_pair, h_far, h_far_pair)
        masked, norm, logp = (pltpu.with_memory_space_constraint(x, pltpu.VMEM) for x in (masked, norm, logp))
        probs, logp = pl.pallas_call(
            finish_kernel,
            out_shape=(jax.ShapeDtypeStruct((rows_dev, length), jnp.float32), jax.ShapeDtypeStruct((1, rows_dev), jnp.float32)),
            in_specs=[vmem_spec] * 3,
            out_specs=(any_spec, any_spec),
            scratch_shapes=[pltpu.VMEM((rows_dev, length), jnp.float32), pltpu.SemaphoreType.DMA((rows_dev // BAND + 1,))],
        )(masked, norm, logp)
        return probs, logp.reshape(rows_dev)

    row_spec = P(('rep', 'vocab'))
    mat_spec = P(('rep', 'vocab'), None)
    return jax.shard_map(device_step, mesh=mesh, in_specs=(mat_spec, P('vocab', None), P('rep'), P('rep'), row_spec), out_specs=(mat_spec, row_spec), check_vma=False)
```
